32 devices in a mesh: groups: 2 (over x), seq: 16 (over z, y, core).
Axes of the slice: x: 2, y: 2, z: 4, core: 2. Of those that a mesh axis runs over, the one named last changes fastest.
Arguments:
- queries: bfloat16 [1024, 2048], P(('groups', 'seq')), parts along dimension 0, may hold values from -132 to 132
- fresh_keys: bfloat16 [1024, 2048], P(('groups', 'seq')), parts along dimension 0, may hold values from -6 to 6
- fresh_values: bfloat16 [1024, 2048], P(('groups', 'seq')), parts along dimension 0, may hold values from -48 to 48
- stale_keys: bfloat16 [1024, 2048], P(('groups', 'seq')), parts along dimension 0, may hold values from -6 to 6
- stale_values: bfloat16 [1024, 2048], P(('groups', 'seq')), parts along dimension 0, may hold values from -48 to 48
- patch_sizes: int32 [8], P('groups'), parts along dimension 0, may hold values from 1 to 256, 512 in all
Outputs:
- attended: bfloat16 [1024, 2048], P(('groups', 'seq')), parts along dimension 0
The draws below stay inside these ranges and needn't reach their ends.
There are 2 independent parts, one for each index of `groups`. The reference program is written for one: setup_inputs(seed, part) draws one part's arguments, and reference() takes and returns one part's arrays. A program takes and returns all parts, laid end to end along the dimension named above; each array names one. Nothing has to cross between parts.
Inputs may be any that keep to these rules, and one draw needn't show every extreme that they name: `patch_sizes`: the patch lengths sum to 512.
All inputs are finite; a program needn't handle non-finite values.
Results may differ from the reference program's by a relative error of at most 0.006.
Values may be sent and summed in bfloat16 or wider, within the bound.
A program may use at most 64 MiB of HBM per device.

```python
import math
import jax
import jax.numpy as jnp
import numpy as np
from jax import lax

H = 16
HD = 128
PATCHES = 4
TOKENS = 512


def base_keys(key):
    return jnp.clip(jax.random.normal(jax.random.fold_in(key, 5), (TOKENS, H * HD), jnp.float32), -6.0, 6.0)


def draw_fresh_keys(key, part):
    return base_keys(key).astype(jnp.bfloat16)


def draw_queries(key, part):
    drawn = jnp.clip(2.0 * jax.random.normal(jax.random.fold_in(key, 6), (TOKENS, H * HD), jnp.float32), -12.0, 12.0)
    return drawn.astype(jnp.bfloat16)


def block_levels(stream_key, shape, cuts, least, high):
    level = 1.0
    for axis_at, shards_of in cuts:
        steps = jax.random.uniform(jax.random.fold_in(jax.random.fold_in(stream_key, 6), axis_at), (shards_of,), jnp.float32, least / len(cuts), high / len(cuts))
        level = level * jnp.repeat(jnp.exp(steps), shape[axis_at] // shards_of).reshape((-1,) + (1,) * (len(shape) - 1 - axis_at))
    return level


def profile(number_of, total, limit, lean):
    loads = [(1 << 20) // math.isqrt(rank ** lean) + 1 for rank in range(2, number_of + 1)]
    spare, holding = total - limit - (number_of - 1), [1] * (number_of - 1)
    while spare > 0:
        free = [i for i in range(number_of - 1) if holding[i] < limit]
        mass, remaining = sum([loads[i] for i in free]), spare
        for i in free:
            more = min(limit - holding[i], max(1, remaining * loads[i] // mass), spare)
            holding[i] = holding[i] + more
            spare = spare - more
    return np.array([limit] + holding)


def ragged_sizes(rng, number_of, total, most, slope):
    if number_of == 2:
        one = jax.random.randint(rng, (), max(1, total - most), min(most, total - 1) + 1)
        return jnp.stack([one, total - one])
    sizes = jnp.asarray(profile(number_of, total, most, slope), jnp.int32)
    couples = (number_of - 1) // 2
    source_of, receiver = sizes[1:1 + 2 * couples:2], sizes[2:2 + 2 * couples:2]
    room = jnp.minimum(source_of - 1, most - receiver)
    moved = jax.random.randint(jax.random.fold_in(rng, 1), (couples,), 0, 1 << 20) % (room + 1)
    sizes = sizes.at[1:1 + 2 * couples:2].set(source_of - moved).at[2:2 + 2 * couples:2].set(receiver + moved)
    return sizes[jax.random.permutation(jax.random.fold_in(rng, 2), number_of)]


def scatter_about(own_key, extent, spread, bound, split=(), held_as=jnp.bfloat16):
    entries = jax.random.normal(own_key, extent, jnp.float32) * spread
    if len(split) > 0:
        entries = block_levels(own_key, extent, split, -0.22, 0.18) * entries
    return jnp.clip(entries, min=-bound, max=bound).astype(held_as)


def setup_inputs(seed: int = 0, part: int = 0) -> dict:
    arg_keys = jax.random.split(jax.random.key(seed), 7)
    part_keys = jax.random.split(jax.random.fold_in(arg_keys[6], part), 7)
    queries = draw_queries(jax.random.fold_in(jax.random.fold_in(arg_keys[6], part), 71), part)
    fresh_keys = draw_fresh_keys(jax.random.fold_in(jax.random.fold_in(arg_keys[6], part), 71), part)
    fresh_values = scatter_about(part_keys[2], (TOKENS, H * HD), 8.0, 48.0, ((0, 16),))
    stale_keys = scatter_about(part_keys[3], (TOKENS, H * HD), 1.0, 6.0, ((0, 16),))
    stale_values = scatter_about(part_keys[4], (TOKENS, H * HD), 8.0, 48.0, ((0, 16),))
    patch_sizes = ragged_sizes(part_keys[5], PATCHES, TOKENS, TOKENS // 2, 1).astype(jnp.int32)
    return dict(queries=queries, fresh_keys=fresh_keys, fresh_values=fresh_values, stale_keys=stale_keys, stale_values=stale_values, patch_sizes=patch_sizes)


def reference(queries, fresh_keys, fresh_values, stale_keys, stale_values, patch_sizes):
    total_rows, columns = queries.shape
    head_size = columns // H
    block_rows = math.gcd(total_rows, 512)
    patch_ends = jnp.cumsum(patch_sizes)[:-1]
    positions = jnp.arange(total_rows, dtype=jnp.int32)
    token_patch = jnp.sum((positions[:, None] >= patch_ends[None, :]).astype(jnp.int32), axis=1)
    score_scale = head_size ** -0.5

    def one_head(head):
        start = (head * head_size).astype(jnp.int32)

        def take(array):
            return lax.dynamic_slice_in_dim(array, start, head_size, 1)

        query_head = take(queries).reshape(-1, block_rows, head_size)
        key_fresh = take(fresh_keys)
        value_fresh = take(fresh_values)
        key_stale = take(stale_keys)
        value_stale = take(stale_values)
        patch_blocks = token_patch.reshape(-1, block_rows)

        def one_block(pair):
            query_block, query_patch = pair
            is_fresh = token_patch[None, :] <= query_patch[:, None]
            fresh_scores = jnp.dot(query_block, key_fresh.T, preferred_element_type=jnp.float32)
            stale_scores = jnp.dot(query_block, key_stale.T, preferred_element_type=jnp.float32)
            scores = jnp.where(is_fresh, fresh_scores, stale_scores) * score_scale
            weights = jnp.exp(scores - jnp.max(scores, axis=1, keepdims=True))
            denominator = jnp.sum(weights, axis=1, keepdims=True)
            rounded = weights.astype(jnp.bfloat16)
            zeroes = jnp.zeros_like(rounded)
            numerator = jnp.dot(jnp.where(is_fresh, rounded, zeroes), value_fresh, preferred_element_type=jnp.float32)
            numerator = numerator + jnp.dot(jnp.where(is_fresh, zeroes, rounded), value_stale, preferred_element_type=jnp.float32)
            return (numerator / denominator).astype(jnp.bfloat16)

        return lax.map(one_block, (query_head, patch_blocks)).reshape(total_rows, head_size)

    heads_out = lax.map(one_head, jnp.arange(H, dtype=jnp.int32))
    return jnp.transpose(heads_out, (1, 0, 2)).reshape(total_rows, columns)
```

```python
import functools

import jax
import jax.numpy as jnp
from jax import lax
from jax.experimental import pallas as pl
from jax.experimental.pallas import tpu as pltpu
from jax.sharding import PartitionSpec as P

H = 16
MESH = pl.DeviceIdType.MESH


def each(count, body):
    if count <= 32:
        for k in range(1, count):
            body(k)
    else:
        lax.fori_loop(1, count, lambda k, c: (body(k), c)[1], 0)


def flipped(me, k, count):
    if count & (count - 1):
        return lax.rem(me + k, count)
    peer, bit = 0, 1
    while bit < count:
        peer = peer + bit * lax.rem(me // bit + k // bit, 2)
        bit *= 2
    return peer


def kernel(
    n, q_ref, fk_ref, sk_ref, fv_ref, sv_ref, sizes_ref, out_ref,
    stage, got_q, got_k, got_v, att, wf_s, ws_s,
    load_sem, own_sem, send_sem, recv_sem, back_send, back_recv,
):
    rows, columns = q_ref.shape
    hd = columns // H
    me = lax.axis_index("seq")
    head = lax.rem(me, H)
    base = me - head
    keys = n * rows
    queries = H * rows

    loads = []
    for i, ref in enumerate((q_ref, fk_ref, sk_ref, fv_ref, sv_ref)):
        c = pltpu.make_async_copy(ref, stage.at[i], load_sem.at[i])
        c.start()
        loads.append(c)

    barrier = pltpu.get_barrier_semaphore()
    each(n, lambda k: pl.semaphore_signal(
        barrier, inc=1, device_id={"seq": flipped(me, k, n)}, device_id_type=MESH))
    pl.semaphore_wait(barrier, n - 1)

    def cols(h):
        return pl.ds(pl.multiple_of(h * hd, hd), hd)

    def at(p):
        return pl.ds(pl.multiple_of(p * rows, rows), rows)

    def views(phase, peer_head, source):
        if phase == 0:
            return stage.at[0, :, cols(peer_head)], got_q.at[at(lax.rem(source, H)), :]
        if phase == 1:
            return stage.at[1:3, :, cols(peer_head)], got_k.at[:, at(source), :]
        return stage.at[3:5, :, cols(peer_head)], got_v.at[:, at(source), :]

    def remote(phase, peer, source, slot):
        src, dst = views(phase, lax.rem(peer, H), source)
        return pltpu.make_async_remote_copy(
            src_ref=src, dst_ref=dst,
            send_sem=send_sem.at[phase, slot], recv_sem=recv_sem.at[phase, slot],
            device_id={"seq": peer}, device_id_type=MESH)

    def own(phase):
        src, dst = views(phase, head, me)
        return pltpu.make_async_copy(src, dst, own_sem.at[phase])

    for phase, needs in ((0, (0,)), (1, (1, 2)), (2, (3, 4))):
        for i in needs:
            loads[i].wait()

        each(H if phase == 0 else n, (lambda k: remote(
            0, base + flipped(head, H - k, H), me, H - k).start()) if phase == 0 else (
            lambda k: remote(phase, flipped(me, n - k, n), me, n - k).start()))
        own(phase).start()

    def arrived(phase, count):
        each(count, lambda k: remote(phase, me, me, k).wait_recv())
        own(phase).wait()

    arrived(0, H)
    arrived(1, n)

    ends, total = [], 0
    for p in range(sizes_ref.shape[0] - 1):
        total = total + sizes_ref[p]
        ends.append(total)

    block = 4 * rows
    scale = hd ** (-0.5)
    contract = (((1,), (1,)), ((), ()))

    def score(b):
        at_b = pl.ds(pl.multiple_of(b * block, block), block)
        token = base * rows + b * block + lax.broadcasted_iota(jnp.int32, (block, 1), 0)
        limit = jnp.full((block, 1), keys, jnp.int32)
        for e in reversed(ends):
            limit = jnp.where(token < e, e, limit)
        fresh = lax.broadcasted_iota(jnp.int32, (block, keys), 1) < limit
        qb = got_q[at_b, :]
        sf = lax.dot_general(qb, got_k[0], contract, preferred_element_type=jnp.float32)
        ss = lax.dot_general(qb, got_k[1], contract, preferred_element_type=jnp.float32)
        s = jnp.where(fresh, sf, ss)
        w = jnp.exp((s - jnp.max(s, axis=1, keepdims=True)) * scale)
        den = jnp.sum(w, axis=1, keepdims=True)
        zero = jnp.zeros_like(w)
        wf_s[at_b, :] = jnp.where(fresh, w, zero).astype(jnp.bfloat16)
        ws_s[at_b, :] = jnp.where(fresh, zero, w).astype(jnp.bfloat16)
        return den

    blocks = queries // block
    dens = [score(b) for b in range(blocks)]

    arrived(2, n)

    def back(j, slot):
        return pltpu.make_async_remote_copy(
            src_ref=att.at[at(j), :], dst_ref=out_ref.at[:, cols(head)],
            send_sem=back_send.at[j], recv_sem=back_recv.at[slot],
            device_id={"seq": base + j}, device_id_type=MESH)

    def back_own(j):
        return pltpu.make_async_copy(att.at[at(j), :], out_ref.at[:, cols(head)], own_sem.at[3])

    for b in range(blocks):
        at_b = pl.ds(b * block, block)
        num = jnp.dot(wf_s[at_b, :], got_v[0], preferred_element_type=jnp.float32)
        num = num + jnp.dot(ws_s[at_b, :], got_v[1], preferred_element_type=jnp.float32)
        att[at_b, :] = (num / dens[b]).astype(jnp.bfloat16)
        for j in range(4 * b, 4 * b + 4):
            pl.when(head != j)(lambda j=j: back(j, head).start())
            pl.when(head == j)(lambda j=j: back_own(j).start())

    each(H, lambda k: remote(0, me, me, k).wait_send())
    each(n, lambda k: remote(1, me, me, k).wait_send())
    each(n, lambda k: remote(2, me, me, k).wait_send())
    for j in range(H):
        @pl.when(head != j)
        def _(j=j):
            back(j, j).wait()
    back_own(0).wait()


def shards(queries, fresh_keys, fresh_values, stale_keys, stale_values, patch_sizes):
    rows, columns = queries.shape
    n = lax.axis_size("seq")
    hd = columns // H
    keys, count = n * rows, H * rows
    dma = pltpu.SemaphoreType.DMA
    any_spec = pl.BlockSpec(memory_space=pl.ANY)
    return pl.pallas_call(
        functools.partial(kernel, n),
        out_shape=jax.ShapeDtypeStruct((rows, columns), queries.dtype),
        in_specs=[any_spec] * 5 + [pl.BlockSpec(memory_space=pltpu.SMEM)],
        out_specs=any_spec,
        scratch_shapes=[
            pltpu.VMEM((5, rows, columns), queries.dtype),
            pltpu.VMEM((count, hd), queries.dtype),
            pltpu.VMEM((2, keys, hd), queries.dtype),
            pltpu.VMEM((2, keys, hd), queries.dtype),
            pltpu.VMEM((count, hd), queries.dtype),
            pltpu.VMEM((count, keys), queries.dtype),
            pltpu.VMEM((count, keys), queries.dtype),
            dma((5,)), dma((4,)), dma((3, n)), dma((3, n)), dma((H,)), dma((H,)),
        ],
        compiler_params=pltpu.CompilerParams(collective_id=0, has_side_effects=True),
    )(queries, fresh_keys, stale_keys, fresh_values, stale_values, patch_sizes)


def solution(mesh):
    spec = P(("groups", "seq"), None)
    return jax.shard_map(
        shards, mesh=mesh, in_specs=(spec,) * 5 + (P("groups"),), out_specs=spec, check_vma=False)
```

```python
import functools

import jax
import jax.numpy as jnp
from jax import lax
from jax.experimental import pallas as pl
from jax.experimental.pallas import tpu as pltpu
from jax.sharding import PartitionSpec as P

H = 16
MESH = pl.DeviceIdType.MESH


def each(count, body):
    if count <= 32:
        for k in range(1, count):
            body(k)
    else:
        lax.fori_loop(1, count, lambda k, c: (body(k), c)[1], 0)


def flipped(me, k, count):
    if count & (count - 1):
        return lax.rem(me + k, count)
    peer, bit = 0, 1
    while bit < count:
        peer = peer + bit * lax.rem(me // bit + k // bit, 2)
        bit *= 2
    return peer


def kernel(
    n, q_ref, fk_ref, sk_ref, fv_ref, sv_ref, sizes_ref, out_ref,
    stage, got_q, got_k, got_v, att, wf_s, ws_s,
    load_sem, own_sem, send_sem, recv_sem, back_send, back_recv,
):
    rows, columns = q_ref.shape
    hd = columns // H
    me = lax.axis_index("seq")
    head = lax.rem(me, H)
    base = me - head
    keys = n * rows
    queries = H * rows

    loads = []
    for i, ref in enumerate((q_ref, fk_ref, sk_ref, fv_ref, sv_ref)):
        c = pltpu.make_async_copy(ref, stage.at[i], load_sem.at[i])
        c.start()
        loads.append(c)

    barrier = pltpu.get_barrier_semaphore()
    each(n, lambda k: pl.semaphore_signal(
        barrier, inc=1, device_id={"seq": flipped(me, k, n)}, device_id_type=MESH))
    pl.semaphore_wait(barrier, n - 1)

    def cols(h):
        return pl.ds(pl.multiple_of(h * hd, hd), hd)

    def at(p):
        return pl.ds(pl.multiple_of(p * rows, rows), rows)

    def views(phase, peer_head, source):
        if phase == 0:
            return stage.at[0, :, cols(peer_head)], got_q.at[at(lax.rem(source, H)), :]
        if phase == 1:
            return stage.at[1:3, :, cols(peer_head)], got_k.at[:, at(source), :]
        return stage.at[3:5, :, cols(peer_head)], got_v.at[:, at(source), :]

    def remote(phase, peer, source, slot):
        src, dst = views(phase, lax.rem(peer, H), source)
        return pltpu.make_async_remote_copy(
            src_ref=src, dst_ref=dst,
            send_sem=send_sem.at[phase, slot], recv_sem=recv_sem.at[phase, slot],
            device_id={"seq": peer}, device_id_type=MESH)

    def own(phase):
        src, dst = views(phase, head, me)
        return pltpu.make_async_copy(src, dst, own_sem.at[phase])

    for phase, needs in ((0, (0,)), (1, (1, 2)), (2, (3, 4))):
        for i in needs:
            loads[i].wait()

        if phase == 0:
            each(H, lambda k: remote(0, base + flipped(head, k, H), me, k).start())
        else:
            each(n, lambda k: remote(phase, flipped(me, k, n), me, k).start())
        own(phase).start()

    def arrived(phase, count):
        each(count, lambda k: remote(phase, me, me, k).wait_recv())
        own(phase).wait()

    arrived(0, H)
    arrived(1, n)

    ends, total = [], 0
    for p in range(sizes_ref.shape[0] - 1):
        total = total + sizes_ref[p]
        ends.append(total)

    block = 4 * rows
    scale = hd ** (-0.5)
    contract = (((1,), (1,)), ((), ()))

    def score(b):
        at_b = pl.ds(pl.multiple_of(b * block, block), block)
        token = base * rows + b * block + lax.broadcasted_iota(jnp.int32, (block, 1), 0)
        limit = jnp.full((block, 1), keys, jnp.int32)
        for e in reversed(ends):
            limit = jnp.where(token < e, e, limit)
        fresh = lax.broadcasted_iota(jnp.int32, (block, keys), 1) < limit
        qb = got_q[at_b, :]
        sf = lax.dot_general(qb, got_k[0], contract, preferred_element_type=jnp.float32)
        ss = lax.dot_general(qb, got_k[1], contract, preferred_element_type=jnp.float32)
        s = jnp.where(fresh, sf, ss)
        w = jnp.exp((s - jnp.max(s, axis=1, keepdims=True)) * scale)
        den = jnp.sum(w, axis=1, keepdims=True)
        zero = jnp.zeros_like(w)
        wf_s[at_b, :] = jnp.where(fresh, w, zero).astype(jnp.bfloat16)
        ws_s[at_b, :] = jnp.where(fresh, zero, w).astype(jnp.bfloat16)
        return den

    order = [flipped(head // 4, k, H // 4) for k in (2, 1, 3, 0)]
    dens = [score(b) for b in order]

    arrived(2, n)

    def back(slot):
        j = flipped(head, slot, H)
        return pltpu.make_async_remote_copy(
            src_ref=att.at[at(j), :], dst_ref=out_ref.at[:, cols(head)],
            send_sem=back_send.at[slot], recv_sem=back_recv.at[slot],
            device_id={"seq": base + j}, device_id_type=MESH)

    back_own = pltpu.make_async_copy(att.at[at(head), :], out_ref.at[:, cols(head)], own_sem.at[3])

    for i, k in enumerate((2, 1, 3, 0)):
        at_b = pl.ds(pl.multiple_of(order[i] * block, block), block)
        num = jnp.dot(wf_s[at_b, :], got_v[0], preferred_element_type=jnp.float32)
        num = num + jnp.dot(ws_s[at_b, :], got_v[1], preferred_element_type=jnp.float32)
        att[at_b, :] = (num / dens[i]).astype(jnp.bfloat16)
        for slot in range(4 * k, 4 * k + 4):
            if slot:
                back(slot).start()
            else:
                back_own.start()

    each(H, lambda k: remote(0, me, me, k).wait_send())
    each(n, lambda k: remote(1, me, me, k).wait_send())
    each(n, lambda k: remote(2, me, me, k).wait_send())
    for slot in range(1, H):
        back(slot).wait()
    back_own.wait()


def shards(queries, fresh_keys, fresh_values, stale_keys, stale_values, patch_sizes):
    rows, columns = queries.shape
    n = lax.axis_size("seq")
    hd = columns // H
    keys, count = n * rows, H * rows
    dma = pltpu.SemaphoreType.DMA
    any_spec = pl.BlockSpec(memory_space=pl.ANY)
    return pl.pallas_call(
        functools.partial(kernel, n),
        out_shape=pltpu.VMEM((rows, columns), queries.dtype),
        in_specs=[any_spec] * 5 + [pl.BlockSpec(memory_space=pltpu.SMEM)],
        out_specs=pl.BlockSpec(memory_space=pltpu.VMEM),
        scratch_shapes=[
            pltpu.VMEM((5, rows, columns), queries.dtype),
            pltpu.VMEM((count, hd), queries.dtype),
            pltpu.VMEM((2, keys, hd), queries.dtype),
            pltpu.VMEM((2, keys, hd), queries.dtype),
            pltpu.VMEM((count, hd), queries.dtype),
            pltpu.VMEM((count, keys), queries.dtype),
            pltpu.VMEM((count, keys), queries.dtype),
            dma((5,)), dma((4,)), dma((3, n)), dma((3, n)), dma((H,)), dma((H,)),
        ],
        compiler_params=pltpu.CompilerParams(collective_id=0, has_side_effects=True),
    )(queries, fresh_keys, stale_keys, fresh_values, stale_values, patch_sizes)


def solution(mesh):
    spec = P(("groups", "seq"), None)
    return jax.shard_map(
        shards, mesh=mesh, in_specs=(spec,) * 5 + (P("groups"),), out_specs=spec, check_vma=False)
```

```python
import functools

import jax
import jax.numpy as jnp
from jax import lax
from jax.experimental import pallas as pl
from jax.experimental.pallas import tpu as pltpu
from jax.sharding import PartitionSpec as P

H = 16
MESH = pl.DeviceIdType.MESH


def each(count, body):
    if count <= 32:
        for k in range(1, count):
            body(k)
    else:
        lax.fori_loop(1, count, lambda k, c: (body(k), c)[1], 0)


def flipped(me, k, count):
    if count & (count - 1):
        return lax.rem(me + k, count)
    peer, bit = 0, 1
    while bit < count:
        peer = peer + bit * lax.rem(me // bit + k // bit, 2)
        bit *= 2
    return peer


def kernel(
    n, fk_ref, sk_ref, fv_ref, sv_ref, q_ref, sizes_ref, out_ref,
    stage, got_q, got_kv, att,
    load_sem, own_sem, send_sem, recv_sem, back_send, back_recv,
):
    rows, columns = q_ref.shape
    hd = columns // H
    me = lax.axis_index("seq")
    head = lax.rem(me, H)
    base = me - head
    keys = n * rows
    queries = H * rows

    loads = []
    for i, ref in enumerate((fk_ref, sk_ref, fv_ref, sv_ref, q_ref)):
        c = pltpu.make_async_copy(ref, stage.at[i], load_sem.at[i])
        c.start()
        loads.append(c)

    barrier = pltpu.get_barrier_semaphore()
    each(n, lambda k: pl.semaphore_signal(
        barrier, inc=1, device_id={"seq": flipped(me, k, n)}, device_id_type=MESH))
    pl.semaphore_wait(barrier, n - 1)

    def cols(h):
        return pl.ds(pl.multiple_of(h * hd, hd), hd)

    def at(p):
        return pl.ds(pl.multiple_of(p * rows, rows), rows)

    def views(phase, peer_head, source):
        if phase == 0:
            return stage.at[0:4, :, cols(peer_head)], got_kv.at[:, at(source), :]
        return stage.at[4, :, cols(peer_head)], got_q.at[at(lax.rem(source, H)), :]

    def remote(phase, peer, source, slot):
        src, dst = views(phase, lax.rem(peer, H), source)
        return pltpu.make_async_remote_copy(
            src_ref=src, dst_ref=dst,
            send_sem=send_sem.at[phase, slot], recv_sem=recv_sem.at[phase, slot],
            device_id={"seq": peer}, device_id_type=MESH)

    def own(phase):
        src, dst = views(phase, head, me)
        return pltpu.make_async_copy(src, dst, own_sem.at[phase])

    for i in range(4):
        loads[i].wait()
    each(n, lambda k: remote(0, flipped(me, k, n), me, k).start())
    own(0).start()
    loads[4].wait()
    each(H, lambda k: remote(1, base + flipped(head, k, H), me, k).start())
    own(1).start()

    ends, total = [], 0
    for p in range(sizes_ref.shape[0] - 1):
        total = total + sizes_ref[p]
        ends.append(total)

    block = 4 * rows
    scale = hd ** (-0.5)
    contract = (((1,), (1,)), ((), ()))

    def attend(b):
        at_b = pl.ds(pl.multiple_of(b * block, block), block)
        token = base * rows + b * block + lax.broadcasted_iota(jnp.int32, (block, 1), 0)
        limit = jnp.full((block, 1), keys, jnp.int32)
        for e in reversed(ends):
            limit = jnp.where(token < e, e, limit)
        fresh = lax.broadcasted_iota(jnp.int32, (block, keys), 1) < limit
        qb = got_q[at_b, :]
        sf = lax.dot_general(qb, got_kv[0], contract, preferred_element_type=jnp.float32)
        ss = lax.dot_general(qb, got_kv[1], contract, preferred_element_type=jnp.float32)
        s = jnp.where(fresh, sf, ss)
        w = jnp.exp((s - jnp.max(s, axis=1, keepdims=True)) * scale)
        den = jnp.sum(w, axis=1, keepdims=True)
        zero = jnp.zeros_like(w)
        wf = jnp.where(fresh, w, zero).astype(jnp.bfloat16)
        ws = jnp.where(fresh, zero, w).astype(jnp.bfloat16)
        num = jnp.dot(wf, got_kv[2], preferred_element_type=jnp.float32)
        num = num + jnp.dot(ws, got_kv[3], preferred_element_type=jnp.float32)
        att[at_b, :] = (num / den).astype(jnp.bfloat16)

    def back(slot):
        j = flipped(head, slot, H)
        return pltpu.make_async_remote_copy(
            src_ref=att.at[at(j), :], dst_ref=out_ref.at[:, cols(head)],
            send_sem=back_send.at[slot], recv_sem=back_recv.at[slot],
            device_id={"seq": base + j}, device_id_type=MESH)

    back_own = pltpu.make_async_copy(att.at[at(head), :], out_ref.at[:, cols(head)], own_sem.at[2])

    each(n, lambda k: remote(0, me, me, k).wait_recv())
    own(0).wait()
    for k in range(H // 4):
        for slot in range(4 * k, 4 * k + 4):
            if slot:
                remote(1, me, me, slot).wait_recv()
            else:
                own(1).wait()
        attend(flipped(head // 4, k, H // 4))
        for slot in range(4 * k, 4 * k + 4):
            if slot:
                back(slot).start()
            else:
                back_own.start()

    each(n, lambda k: remote(0, me, me, k).wait_send())
    each(H, lambda k: remote(1, me, me, k).wait_send())
    for slot in range(1, H):
        back(slot).wait()
    back_own.wait()


def shards(queries, fresh_keys, fresh_values, stale_keys, stale_values, patch_sizes):
    rows, columns = queries.shape
    n = lax.axis_size("seq")
    hd = columns // H
    keys, count = n * rows, H * rows
    dma = pltpu.SemaphoreType.DMA
    any_spec = pl.BlockSpec(memory_space=pl.ANY)
    return pl.pallas_call(
        functools.partial(kernel, n),
        out_shape=pltpu.VMEM((rows, columns), queries.dtype),
        in_specs=[any_spec] * 5 + [pl.BlockSpec(memory_space=pltpu.SMEM)],
        out_specs=pl.BlockSpec(memory_space=pltpu.VMEM),
        scratch_shapes=[
            pltpu.VMEM((5, rows, columns), queries.dtype),
            pltpu.VMEM((count, hd), queries.dtype),
            pltpu.VMEM((4, keys, hd), queries.dtype),
            pltpu.VMEM((count, hd), queries.dtype),
            dma((5,)), dma((3,)), dma((2, n)), dma((2, n)), dma((H,)), dma((H,)),
        ],
        compiler_params=pltpu.CompilerParams(collective_id=0, has_side_effects=True),
    )(fresh_keys, stale_keys, fresh_values, stale_values, queries, patch_sizes)


def solution(mesh):
    spec = P(("groups", "seq"), None)
    return jax.shard_map(
        shards, mesh=mesh, in_specs=(spec,) * 5 + (P("groups"),), out_specs=spec, check_vma=False)
```

```python
import functools

import jax
import jax.numpy as jnp
from jax import lax
from jax.experimental import pallas as pl
from jax.experimental.pallas import tpu as pltpu
from jax.sharding import PartitionSpec as P

H = 16
MESH = pl.DeviceIdType.MESH


def each(count, body):
    if count <= 32:
        for k in range(1, count):
            body(k)
    else:
        lax.fori_loop(1, count, lambda k, c: (body(k), c)[1], 0)


def flipped(me, k, count):
    if count & (count - 1):
        return lax.rem(me + k, count)
    peer, bit = 0, 1
    while bit < count:
        peer = peer + bit * lax.rem(me // bit + k // bit, 2)
        bit *= 2
    return peer


def kernel(
    n, fk_ref, sk_ref, fv_ref, sv_ref, q_ref, sizes_ref, out_ref,
    stage, got_q, got_kv, att,
    load_sem, own_sem, send_sem, recv_sem, back_send, back_recv,
):
    rows, columns = q_ref.shape
    hd = columns // H
    me = lax.axis_index("seq")
    head = lax.rem(me, H)
    base = me - head
    keys = n * rows
    queries = H * rows

    loads = []
    for i, ref in enumerate((fk_ref, sk_ref, fv_ref, sv_ref, q_ref)):
        c = pltpu.make_async_copy(ref, stage.at[i], load_sem.at[i])
        c.start()
        loads.append(c)

    barrier = pltpu.get_barrier_semaphore()
    each(n, lambda k: pl.semaphore_signal(
        barrier, inc=1, device_id={"seq": flipped(me, k, n)}, device_id_type=MESH))
    pl.semaphore_wait(barrier, n - 1)

    def cols(h):
        return pl.ds(pl.multiple_of(h * hd, hd), hd)

    def at(p):
        return pl.ds(pl.multiple_of(p * rows, rows), rows)

    def views(phase, peer_head, source):
        if phase == 0:
            return stage.at[0:4, :, cols(peer_head)], got_kv.at[:, at(source), :]
        return stage.at[4, :, cols(peer_head)], got_q.at[at(lax.rem(source, H)), :]

    def remote(phase, peer, source, slot):
        src, dst = views(phase, lax.rem(peer, H), source)
        return pltpu.make_async_remote_copy(
            src_ref=src, dst_ref=dst,
            send_sem=send_sem.at[phase, slot], recv_sem=recv_sem.at[phase, slot],
            device_id={"seq": peer}, device_id_type=MESH)

    def own(phase):
        src, dst = views(phase, head, me)
        return pltpu.make_async_copy(src, dst, own_sem.at[phase])

    loads[4].wait()
    each(H, lambda k: remote(1, base + flipped(head, k, H), me, k).start())
    own(1).start()
    for i in range(4):
        loads[i].wait()
    each(n, lambda k: remote(0, flipped(me, k, n), me, k).start())
    own(0).start()

    ends, total = [], 0
    for p in range(sizes_ref.shape[0] - 1):
        total = total + sizes_ref[p]
        ends.append(total)

    block = 4 * rows
    scale = hd ** (-0.5)
    contract = (((1,), (1,)), ((), ()))

    def attend(b):
        at_b = pl.ds(pl.multiple_of(b * block, block), block)
        token = base * rows + b * block + lax.broadcasted_iota(jnp.int32, (block, 1), 0)
        limit = jnp.full((block, 1), keys, jnp.int32)
        for e in reversed(ends):
            limit = jnp.where(token < e, e, limit)
        fresh = lax.broadcasted_iota(jnp.int32, (block, keys), 1) < limit
        qb = got_q[at_b, :]
        sf = lax.dot_general(qb, got_kv[0], contract, preferred_element_type=jnp.float32)
        ss = lax.dot_general(qb, got_kv[1], contract, preferred_element_type=jnp.float32)
        s = jnp.where(fresh, sf, ss)
        w = jnp.exp((s - jnp.max(s, axis=1, keepdims=True)) * scale)
        den = jnp.sum(w, axis=1, keepdims=True)
        zero = jnp.zeros_like(w)
        wf = jnp.where(fresh, w, zero).astype(jnp.bfloat16)
        ws = jnp.where(fresh, zero, w).astype(jnp.bfloat16)
        num = jnp.dot(wf, got_kv[2], preferred_element_type=jnp.float32)
        num = num + jnp.dot(ws, got_kv[3], preferred_element_type=jnp.float32)
        att[at_b, :] = (num / den).astype(jnp.bfloat16)

    def back(slot):
        j = flipped(head, slot, H)
        return pltpu.make_async_remote_copy(
            src_ref=att.at[at(j), :], dst_ref=out_ref.at[:, cols(head)],
            send_sem=back_send.at[slot], recv_sem=back_recv.at[slot],
            device_id={"seq": base + j}, device_id_type=MESH)

    back_own = pltpu.make_async_copy(att.at[at(head), :], out_ref.at[:, cols(head)], own_sem.at[2])

    each(n, lambda k: remote(0, me, me, k).wait_recv())
    own(0).wait()
    for k in (2, 3, 1, 0):
        for slot in range(4 * k, 4 * k + 4):
            if slot:
                remote(1, me, me, slot).wait_recv()
            else:
                own(1).wait()
        attend(flipped(head // 4, k, H // 4))
        for slot in range(4 * k, 4 * k + 4):
            if slot:
                back(slot).start()
            else:
                back_own.start()

    each(n, lambda k: remote(0, me, me, k).wait_send())
    each(H, lambda k: remote(1, me, me, k).wait_send())
    for slot in range(1, H):
        back(slot).wait()
    back_own.wait()


def shards(queries, fresh_keys, fresh_values, stale_keys, stale_values, patch_sizes):
    rows, columns = queries.shape
    n = lax.axis_size("seq")
    hd = columns // H
    keys, count = n * rows, H * rows
    dma = pltpu.SemaphoreType.DMA
    any_spec = pl.BlockSpec(memory_space=pl.ANY)
    return pl.pallas_call(
        functools.partial(kernel, n),
        out_shape=pltpu.VMEM((rows, columns), queries.dtype),
        in_specs=[any_spec] * 5 + [pl.BlockSpec(memory_space=pltpu.SMEM)],
        out_specs=pl.BlockSpec(memory_space=pltpu.VMEM),
        scratch_shapes=[
            pltpu.VMEM((5, rows, columns), queries.dtype),
            pltpu.VMEM((count, hd), queries.dtype),
            pltpu.VMEM((4, keys, hd), queries.dtype),
            pltpu.VMEM((count, hd), queries.dtype),
            dma((5,)), dma((3,)), dma((2, n)), dma((2, n)), dma((H,)), dma((H,)),
        ],
        compiler_params=pltpu.CompilerParams(collective_id=0, has_side_effects=True),
    )(fresh_keys, stale_keys, fresh_values, stale_values, queries, patch_sizes)


def solution(mesh):
    spec = P(("groups", "seq"), None)
    return jax.shard_map(
        shards, mesh=mesh, in_specs=(spec,) * 5 + (P("groups"),), out_specs=spec, check_vma=False)
```

```python
import functools

import jax
import jax.numpy as jnp
from jax import lax
from jax.experimental import pallas as pl
from jax.experimental.pallas import tpu as pltpu
from jax.sharding import PartitionSpec as P

H = 16
MESH = pl.DeviceIdType.MESH


def each(count, body):
    if count <= 32:
        for k in range(1, count):
            body(k)
    else:
        lax.fori_loop(1, count, lambda k, c: (body(k), c)[1], 0)


def flipped(me, k, count):
    if count & (count - 1):
        return lax.rem(me + k, count)
    peer, bit = 0, 1
    while bit < count:
        peer = peer + bit * lax.rem(me // bit + k // bit, 2)
        bit *= 2
    return peer


def kernel(
    n, fk_ref, sk_ref, fv_ref, sv_ref, q_ref, sizes_ref, out_ref,
    stage, got_q, got_kv, att,
    load_sem, own_sem, send_sem, recv_sem, back_send, back_recv, here,
):
    rows, columns = q_ref.shape
    hd = columns // H
    me = lax.axis_index("seq")
    head = lax.rem(me, H)
    base = me - head
    keys = n * rows
    queries = H * rows

    loads = []
    for i, ref in enumerate((fk_ref, sk_ref, fv_ref, sv_ref, q_ref)):
        c = pltpu.make_async_copy(ref, stage.at[i], load_sem.at[i])
        c.start()
        loads.append(c)

    def cols(h):
        return pl.ds(pl.multiple_of(h * hd, hd), hd)

    def at(p):
        return pl.ds(pl.multiple_of(p * rows, rows), rows)

    def views(phase, peer_head, source):
        if phase == 0:
            return stage.at[0:4, :, cols(peer_head)], got_kv.at[:, at(source), :]
        return stage.at[4, :, cols(peer_head)], got_q.at[at(lax.rem(source, H)), :]

    def remote(phase, peer, source, slot):
        src, dst = views(phase, lax.rem(peer, H), source)
        return pltpu.make_async_remote_copy(
            src_ref=src, dst_ref=dst,
            send_sem=send_sem.at[phase, slot], recv_sem=recv_sem.at[phase, slot],
            device_id={"seq": peer}, device_id_type=MESH)

    def own(phase):
        src, dst = views(phase, head, me)
        return pltpu.make_async_copy(src, dst, own_sem.at[phase])

    quarter = n // 4
    half = n // 2
    lane = me // quarter
    inner = lax.rem(lane + 1, 4) >= 2
    like = [k for k in range(1, n) if k // quarter in (0, 3)]
    cross = [k for k in range(1, n) if k // quarter in (1, 2)]
    barrier = pltpu.get_barrier_semaphore()

    def greet(sem, ks):
        for k in ks:
            pl.semaphore_signal(
                sem, inc=1, device_id={"seq": flipped(me, k, n)}, device_id_type=MESH)

    def send(ks):
        for k in ks:
            if k < H:
                remote(1, flipped(me, k, n), me, k).start()
        for k in ks:
            remote(0, flipped(me, k, n), me, k).start()

    def loaded():
        for load in loads:
            load.wait()

    @pl.when(inner)
    def _():
        greet(barrier, like + cross)
        pl.semaphore_wait(barrier, half - 1)
        loaded()
        send(like)
        pl.semaphore_wait(here, half)
        greet(here, [quarter])
        send(cross)

    @pl.when(jnp.logical_not(inner))
    def _():
        pl.semaphore_wait(barrier, half)
        greet(here, cross)
        loaded()
        send(cross)
        pl.semaphore_wait(here, 1)
        send(like)

    own(1).start()
    own(0).start()

    ends, total = [], 0
    for p in range(sizes_ref.shape[0] - 1):
        total = total + sizes_ref[p]
        ends.append(total)

    block = 4 * rows
    scale = hd ** (-0.5)
    contract = (((1,), (1,)), ((), ()))

    def attend(b):
        at_b = pl.ds(pl.multiple_of(b * block, block), block)
        token = base * rows + b * block + lax.broadcasted_iota(jnp.int32, (block, 1), 0)
        limit = jnp.full((block, 1), keys, jnp.int32)
        for e in reversed(ends):
            limit = jnp.where(token < e, e, limit)
        fresh = lax.broadcasted_iota(jnp.int32, (block, keys), 1) < limit
        qb = got_q[at_b, :]
        sf = lax.dot_general(qb, got_kv[0], contract, preferred_element_type=jnp.float32)
        ss = lax.dot_general(qb, got_kv[1], contract, preferred_element_type=jnp.float32)
        s = jnp.where(fresh, sf, ss)
        w = jnp.exp((s - jnp.max(s, axis=1, keepdims=True)) * scale)
        den = jnp.sum(w, axis=1, keepdims=True)
        zero = jnp.zeros_like(w)
        wf = jnp.where(fresh, w, zero).astype(jnp.bfloat16)
        ws = jnp.where(fresh, zero, w).astype(jnp.bfloat16)
        num = jnp.dot(wf, got_kv[2], preferred_element_type=jnp.float32)
        num = num + jnp.dot(ws, got_kv[3], preferred_element_type=jnp.float32)
        att[at_b, :] = (num / den).astype(jnp.bfloat16)

    def back(slot):
        j = flipped(head, slot, H)
        return pltpu.make_async_remote_copy(
            src_ref=att.at[at(j), :], dst_ref=out_ref.at[:, cols(head)],
            send_sem=back_send.at[slot], recv_sem=back_recv.at[slot],
            device_id={"seq": base + j}, device_id_type=MESH)

    back_own = pltpu.make_async_copy(att.at[at(head), :], out_ref.at[:, cols(head)], own_sem.at[2])

    each(n, lambda k: remote(0, me, me, k).wait_recv())
    own(0).wait()
    for k in (2, 3, 1, 0):
        for slot in range(4 * k, 4 * k + 4):
            if slot:
                remote(1, me, me, slot).wait_recv()
            else:
                own(1).wait()
        attend(flipped(head // 4, k, H // 4))
        for slot in range(4 * k, 4 * k + 4):
            if slot:
                back(slot).start()
            else:
                back_own.start()

    each(n, lambda k: remote(0, me, me, k).wait_send())
    each(H, lambda k: remote(1, me, me, k).wait_send())
    for slot in range(1, H):
        back(slot).wait()
    back_own.wait()


def shards(queries, fresh_keys, fresh_values, stale_keys, stale_values, patch_sizes):
    rows, columns = queries.shape
    n = lax.axis_size("seq")
    hd = columns // H
    keys, count = n * rows, H * rows
    dma = pltpu.SemaphoreType.DMA
    any_spec = pl.BlockSpec(memory_space=pl.ANY)
    return pl.pallas_call(
        functools.partial(kernel, n),
        out_shape=pltpu.VMEM((rows, columns), queries.dtype),
        in_specs=[any_spec] * 5 + [pl.BlockSpec(memory_space=pltpu.SMEM)],
        out_specs=pl.BlockSpec(memory_space=pltpu.VMEM),
        scratch_shapes=[
            pltpu.VMEM((5, rows, columns), queries.dtype),
            pltpu.VMEM((count, hd), queries.dtype),
            pltpu.VMEM((4, keys, hd), queries.dtype),
            pltpu.VMEM((count, hd), queries.dtype),
            dma((5,)), dma((3,)), dma((2, n)), dma((2, n)), dma((H,)), dma((H,)), pltpu.SemaphoreType.REGULAR,
        ],
        compiler_params=pltpu.CompilerParams(collective_id=0, has_side_effects=True),
    )(fresh_keys, stale_keys, fresh_values, stale_values, queries, patch_sizes)


def solution(mesh):
    spec = P(("groups", "seq"), None)
    return jax.shard_map(
        shards, mesh=mesh, in_specs=(spec,) * 5 + (P("groups"),), out_specs=spec, check_vma=False)
```
